32 devices in a mesh: gx: 8 (over z, y), gy: 4 (over x, core).
Axes of the slice: x: 2, y: 2, z: 4, core: 2. Of those that a mesh axis runs over, the one named last changes fastest.
Arguments:
- fine_nodes: bfloat16 [32768, 512], P(('gx', 'gy')), may hold values from -6 to 6
- edge_latent: bfloat16 [196608, 512], P(('gx', 'gy')), may hold values from -6 to 6
- boundary: int32 [4096], P(('gx', 'gy')), may hold values from 0 to 1023, as said below
- fine_src: int32 [196608], P(('gx', 'gy')), may hold values from 0 to 2175, as said below
- fine_dst: int32 [196608], P(('gx', 'gy')), may hold values from 0 to 1023
- parent_one: int32 [32768], P(('gx', 'gy')), may hold values from 0 to 831, as said below
- weight_one: bfloat16 [32768], P(('gx', 'gy')), may hold values from 0.049804688 to 0.29882812
- coarse_src_one: int32 [49152], P(('gx', 'gy')), may hold values from 0 to 831, as said below
- coarse_dst_one: int32 [49152], P(('gx', 'gy')), may hold values from 0 to 255
- parent_two: int32 [8192], P(('gx', 'gy')), may hold values from 0 to 351, as said below
- weight_two: bfloat16 [8192], P(('gx', 'gy')), may hold values from 0.099609375 to 0.5
- coarse_src_two: int32 [12288], P(('gx', 'gy')), may hold values from 0 to 351, as said below
- coarse_dst_two: int32 [12288], P(('gx', 'gy')), may hold values from 0 to 63
- fine_message_in: bfloat16 [1536, 512], replicated, may hold values from -0.15625 to 0.15625
- fine_message_out: bfloat16 [512, 512], replicated, may hold values from -0.25 to 0.25
- fine_message_gain: bfloat16 [512], replicated, may hold values from 0.25 to 1.75
- fine_update_in: bfloat16 [1024, 512], replicated, may hold values from -0.1875 to 0.1875
- fine_update_out: bfloat16 [512, 512], replicated, may hold values from -0.25 to 0.25
- fine_update_gain: bfloat16 [512], replicated, may hold values from 0.25 to 1.75
- coarse_message_in: bfloat16 [1024, 512], replicated, may hold values from -0.1875 to 0.1875
- coarse_message_out: bfloat16 [512, 512], replicated, may hold values from -0.25 to 0.25
- coarse_message_gain: bfloat16 [512], replicated, may hold values from 0.25 to 1.75
- coarse_update_in: bfloat16 [1024, 512], replicated, may hold values from -0.1875 to 0.1875
- coarse_update_out: bfloat16 [512, 512], replicated, may hold values from -0.25 to 0.25
- coarse_update_gain: bfloat16 [512], replicated, may hold values from 0.25 to 1.75
Outputs:
- fine_out: bfloat16 [32768, 512], P(('gx', 'gy'))
The draws below stay inside these ranges and needn't reach their ends.
Inputs may be any that keep to these rules, and one draw needn't show every extreme that they name: `boundary`: each device's 128 entries are distinct local row numbers of its own fine nodes. `fine_src`: an entry below 1024 is a local row of the edge's own device; an entry 1024 + k * 128 + r names boundary row r of the device at grid offset (k // 3 - 1, k % 3 - 1) along (gx, gy), with wrap; k is never 4. `parent_one`: an entry below 256 is a first coarse level row of the fine node's own device; an entry 256 + k * 64 + r names rim row r of the device at grid offset (k // 3 - 1, k % 3 - 1) along (gx, gy), with wrap; k is never 4. `coarse_src_one`: an entry below 256 is a first coarse level row of the edge's own device; an entry 256 + k * 64 + r names rim row r of the device at grid offset (k // 3 - 1, k % 3 - 1) along (gx, gy), with wrap; k is never 4. `parent_two`: an entry below 64 is a second coarse level row of the node's own device; an entry 64 + k * 32 + r names rim row r of the device at grid offset (k // 3 - 1, k % 3 - 1) along (gx, gy), with wrap; k is never 4. `coarse_src_two`: an entry below 64 is a second coarse level row of the edge's own device; an entry 64 + k * 32 + r names rim row r of the device at grid offset (k // 3 - 1, k % 3 - 1) along (gx, gy), with wrap; k is never 4.
All inputs are finite; a program needn't handle non-finite values.
Results may differ from the reference program's by a relative error of at most 0.012.
Values may be sent and summed in bfloat16 or wider, within the bound.
No kernel may reach another device: no remote copies, remote signals or barrier semaphores. Data moves between devices by JAX's collectives and lax.ppermute only.
A program may use at most 128 MiB of HBM per device.

```python
import math
import jax
import jax.numpy as jnp
from jax import lax

D = 512
NF_DEV = 1024
BND = 128
E_DEV = 6144
NC1_DEV = 256
NC2_DEV = 64
CB1 = 64
CB2 = 32
E1_DEV = 1536
E2_DEV = 384
NF = 32768
NC1 = 8192
NC2 = 2048
N_GX = 8
N_GY = 4


def rim_numbers(key, count, local_count, rim_count, outward):
    streams = jax.random.split(key, 4)
    inside = jax.random.randint(streams[0], (count,), 0, local_count)
    sector = jax.random.randint(streams[1], (count,), 0, 8)
    sector = sector + (sector >= 4).astype(jnp.int32)
    beyond = local_count + sector * rim_count + jax.random.randint(streams[2], (count,), 0, rim_count)
    chosen = jax.random.randint(streams[3], (count,), 0, 8) < outward
    return jnp.where(chosen, beyond, inside).astype(jnp.int32)


def draw_boundary(key, part):
    scores = jax.random.randint(jax.random.fold_in(key, 11), (N_GX * N_GY, NF_DEV), 0, 65536)
    scores = scores * NF_DEV + jnp.arange(NF_DEV, dtype=jnp.int32)[None, :]
    ordering = jnp.argsort(scores, axis=1)
    return ordering[:, :BND].reshape(-1).astype(jnp.int32)


def draw_fine_src(key, part):
    return rim_numbers(jax.random.fold_in(key, 23), N_GX * N_GY * E_DEV, NF_DEV, BND, 4)


def draw_parent_one(key, part):
    return rim_numbers(jax.random.fold_in(key, 31), N_GX * N_GY * NF_DEV, NC1_DEV, CB1, 4)


def draw_coarse_src_one(key, part):
    return rim_numbers(jax.random.fold_in(key, 37), N_GX * N_GY * E1_DEV, NC1_DEV, CB1, 4)


def draw_parent_two(key, part):
    return rim_numbers(jax.random.fold_in(key, 41), N_GX * N_GY * NC1_DEV, NC2_DEV, CB2, 5)


def draw_coarse_src_two(key, part):
    return rim_numbers(jax.random.fold_in(key, 43), N_GX * N_GY * E2_DEV, NC2_DEV, CB2, 4)


def touch_ends(result, own_key, least, high):
    longest = result.shape.index(max(result.shape))
    spots = []
    for shift in (0, 1):
        where = [jax.random.randint(jax.random.fold_in(own_key, axis), (), 0, length) for axis, length in enumerate(result.shape)]
        where[longest] = (where[longest] + shift) % result.shape[longest]
        spots.append(tuple(where))
    return result.at[spots[0]].set(least).at[spots[1]].set(high)


def steps_of(key, extent, shards, low, top_value):
    factor_of, own = 1.0, jax.random.fold_in(key, 6)
    for dim, shards_of in shards:
        heights = jnp.exp(jax.random.uniform(jax.random.fold_in(own, dim), (shards_of,), jnp.float32, low / len(shards), top_value / len(shards)))
        factor_of = factor_of * jnp.repeat(heights, extent[dim] // shards_of).reshape([-1 if axis == dim else 1 for axis in range(len(extent))])
    return factor_of


def normal_values(rng, dims, width, reach, cuts=(), held_as=jnp.bfloat16):
    factor_of = steps_of(rng, dims, cuts, -0.22, 0.18) if cuts else 1.0
    result = jax.random.normal(rng, dims, jnp.float32) * width * factor_of
    return jnp.minimum(jnp.maximum(result, -reach), reach).astype(held_as)


def setup_inputs(seed: int = 0) -> dict:
    seeds = jax.random.split(jax.random.key(seed), 26)
    fine_nodes = normal_values(seeds[0], (NF, D), 1.0, 6.0, ((0, 32),))
    edge_latent = normal_values(seeds[1], (N_GX * N_GY * E_DEV, D), 1.0, 6.0, ((0, 32),))
    boundary = draw_boundary(jax.random.fold_in(seeds[25], 71), 0)
    fine_src = draw_fine_src(jax.random.fold_in(seeds[25], 71), 0)
    fine_dst = touch_ends(jax.random.randint(seeds[4], (N_GX * N_GY * E_DEV,), 0, NF_DEV), jax.random.fold_in(seeds[4], 1), 0, NF_DEV - 1).astype(jnp.int32)
    parent_one = draw_parent_one(jax.random.fold_in(seeds[25], 71), 0)
    weight_one = jnp.clip(jnp.exp(math.log(0.29882812) - 1.7917595 * jax.random.uniform(seeds[6], (NF,), jnp.float32) ** steps_of(seeds[6], (NF,), ((0, 32),), -0.2, 0.2)), 0.049804688, 0.29882812).astype(jnp.bfloat16)
    coarse_src_one = draw_coarse_src_one(jax.random.fold_in(seeds[25], 71), 0)
    coarse_dst_one = touch_ends(jax.random.randint(seeds[8], (N_GX * N_GY * E1_DEV,), 0, NC1_DEV), jax.random.fold_in(seeds[8], 1), 0, NC1_DEV - 1).astype(jnp.int32)
    parent_two = draw_parent_two(jax.random.fold_in(seeds[25], 71), 0)
    weight_two = jnp.clip(jnp.exp(math.log(0.5) - 1.6133518 * jax.random.uniform(seeds[10], (NC1,), jnp.float32) ** steps_of(seeds[10], (NC1,), ((0, 32),), -0.2, 0.2)), 0.099609375, 0.5).astype(jnp.bfloat16)
    coarse_src_two = draw_coarse_src_two(jax.random.fold_in(seeds[25], 71), 0)
    coarse_dst_two = touch_ends(jax.random.randint(seeds[12], (N_GX * N_GY * E2_DEV,), 0, NC2_DEV), jax.random.fold_in(seeds[12], 1), 0, NC2_DEV - 1).astype(jnp.int32)
    fine_message_in = normal_values(seeds[13], (3 * D, D), (3 * D) ** -0.5, 0.15625)
    fine_message_out = normal_values(seeds[14], (D, D), D ** -0.5, 0.25)
    fine_message_gain = jnp.clip(1.0 + 0.15 * jax.random.normal(seeds[15], (D,), jnp.float32), 0.25, 1.75).astype(jnp.bfloat16)
    fine_update_in = normal_values(seeds[16], (2 * D, D), (2 * D) ** -0.5, 0.1875)
    fine_update_out = normal_values(seeds[17], (D, D), D ** -0.5, 0.25)
    fine_update_gain = jnp.clip(1.0 + 0.15 * jax.random.normal(seeds[18], (D,), jnp.float32), 0.25, 1.75).astype(jnp.bfloat16)
    coarse_message_in = normal_values(seeds[19], (2 * D, D), (2 * D) ** -0.5, 0.1875)
    coarse_message_out = normal_values(seeds[20], (D, D), D ** -0.5, 0.25)
    coarse_message_gain = jnp.clip(1.0 + 0.15 * jax.random.normal(seeds[21], (D,), jnp.float32), 0.25, 1.75).astype(jnp.bfloat16)
    coarse_update_in = normal_values(seeds[22], (2 * D, D), (2 * D) ** -0.5, 0.1875)
    coarse_update_out = normal_values(seeds[23], (D, D), D ** -0.5, 0.25)
    coarse_update_gain = jnp.clip(1.0 + 0.15 * jax.random.normal(seeds[24], (D,), jnp.float32), 0.25, 1.75).astype(jnp.bfloat16)
    return dict(fine_nodes=fine_nodes, edge_latent=edge_latent, boundary=boundary, fine_src=fine_src, fine_dst=fine_dst, parent_one=parent_one, weight_one=weight_one, coarse_src_one=coarse_src_one, coarse_dst_one=coarse_dst_one, parent_two=parent_two, weight_two=weight_two, coarse_src_two=coarse_src_two, coarse_dst_two=coarse_dst_two, fine_message_in=fine_message_in, fine_message_out=fine_message_out, fine_message_gain=fine_message_gain, fine_update_in=fine_update_in, fine_update_out=fine_update_out, fine_update_gain=fine_update_gain, coarse_message_in=coarse_message_in, coarse_message_out=coarse_message_out, coarse_message_gain=coarse_message_gain, coarse_update_in=coarse_update_in, coarse_update_out=coarse_update_out, coarse_update_gain=coarse_update_gain)


def normed(preact, scales):
    average = lax.optimization_barrier(jnp.mean(preact, axis=-1, keepdims=True))
    centred = preact - average
    spread = lax.optimization_barrier(jnp.mean(centred * centred, axis=-1, keepdims=True))
    return centred * lax.rsqrt(spread + 1e-05) * scales.astype(jnp.float32)

def network(inputs, project_in, project_out, scales):
    preact = jnp.dot(inputs, project_in, preferred_element_type=jnp.float32)
    hidden = jax.nn.silu(preact).astype(jnp.bfloat16)
    return normed(jnp.dot(hidden, project_out, preferred_element_type=jnp.float32), scales)

def to_global(numbers, per_device, local_count, rim_count):
    owners = jnp.arange(numbers.shape[0], dtype=jnp.int32) // per_device
    first_coord = owners // N_GY
    second_coord = owners % N_GY
    beyond = jnp.maximum(numbers - local_count, 0)
    sector = beyond // rim_count
    within = beyond % rim_count
    neighbour = (first_coord + sector // 3 - 1) % N_GX * N_GY + (second_coord + sector % 3 - 1) % N_GY
    return jnp.where(numbers < local_count, owners * local_count + numbers, neighbour * local_count + within).astype(jnp.int32)

def level_pass(states, sources, targets, node_count, message_in, message_out, message_gain, update_in, update_out, update_gain):
    inputs = jnp.concatenate([states[sources], states[targets]], axis=1)
    messages = network(inputs, message_in, message_out, message_gain).astype(jnp.bfloat16)
    incoming = jax.ops.segment_sum(messages.astype(jnp.float32), targets, num_segments=node_count).astype(jnp.bfloat16)
    update = network(jnp.concatenate([states, incoming], axis=1), update_in, update_out, update_gain)
    return (states.astype(jnp.float32) + update).astype(jnp.bfloat16)

def restrict(states, parents, weights, node_count):
    terms = weights.astype(jnp.float32)[:, None] * states.astype(jnp.float32)
    return jax.ops.segment_sum(terms, parents, num_segments=node_count).astype(jnp.bfloat16)

def reference(fine_nodes, edge_latent, boundary, fine_src, fine_dst, parent_one, weight_one, coarse_src_one, coarse_dst_one, parent_two, weight_two, coarse_src_two, coarse_dst_two, fine_message_in, fine_message_out, fine_message_gain, fine_update_in, fine_update_out, fine_update_gain, coarse_message_in, coarse_message_out, coarse_message_gain, coarse_update_in, coarse_update_out, coarse_update_gain):
    devices = N_GX * N_GY
    features = fine_nodes.shape[1]
    parent_one_global = to_global(parent_one, NF_DEV, NC1_DEV, CB1)
    coarse_src_one_global = to_global(coarse_src_one, E1_DEV, NC1_DEV, CB1)
    parent_two_global = to_global(parent_two, NC1_DEV, NC2_DEV, CB2)
    coarse_src_two_global = to_global(coarse_src_two, E2_DEV, NC2_DEV, CB2)
    device_ids = jnp.arange(devices, dtype=jnp.int32)
    flat_rows = (device_ids[:, None] * NF_DEV + boundary.reshape(devices, BND)).reshape(-1)
    chosen = fine_nodes[flat_rows].reshape(N_GX, N_GY, BND, features)
    blocks = []
    for offset_x in range(3):
        for offset_y in range(3):
            blocks.append(jnp.roll(chosen, (1 - offset_x, 1 - offset_y), axis=(0, 1)))
    beside_all = jnp.stack(blocks, axis=2).reshape(devices, 9 * BND, features)

    def one_device(packed):
        nodes, neighbours, latent, sources, targets = packed
        extended = jnp.concatenate([nodes, neighbours], axis=0)
        inputs = jnp.concatenate([extended[sources], nodes[targets], latent], axis=1)
        messages = network(inputs, fine_message_in, fine_message_out, fine_message_gain).astype(jnp.bfloat16)
        incoming = jax.ops.segment_sum(messages.astype(jnp.float32), targets, num_segments=NF_DEV).astype(jnp.bfloat16)
        update = network(jnp.concatenate([nodes, incoming], axis=1), fine_update_in, fine_update_out, fine_update_gain)
        return (nodes.astype(jnp.float32) + update).astype(jnp.bfloat16)
    fine_new = lax.map(one_device, (fine_nodes.reshape(devices, NF_DEV, features), beside_all, edge_latent.reshape(devices, E_DEV, features), fine_src.reshape(devices, E_DEV), fine_dst.reshape(devices, E_DEV)))
    fine_new = fine_new.reshape(devices * NF_DEV, features)
    level_one = restrict(fine_new, parent_one_global, weight_one, NC1)
    owner_one = jnp.arange(devices * E1_DEV, dtype=jnp.int32) // E1_DEV * NC1_DEV
    level_one_new = level_pass(level_one, coarse_src_one_global, owner_one + coarse_dst_one, NC1, coarse_message_in, coarse_message_out, coarse_message_gain, coarse_update_in, coarse_update_out, coarse_update_gain)
    level_two = restrict(level_one_new, parent_two_global, weight_two, NC2)
    owner_two = jnp.arange(devices * E2_DEV, dtype=jnp.int32) // E2_DEV * NC2_DEV
    level_two_new = level_pass(level_two, coarse_src_two_global, owner_two + coarse_dst_two, NC2, coarse_message_in, coarse_message_out, coarse_message_gain, coarse_update_in, coarse_update_out, coarse_update_gain)
    level_one_final = (level_one_new.astype(jnp.float32) + level_two_new[parent_two_global].astype(jnp.float32)).astype(jnp.bfloat16)
    return (fine_new.astype(jnp.float32) + level_one_final[parent_one_global].astype(jnp.float32)).astype(jnp.bfloat16)
```

```python
import jax
import jax.numpy as jnp
from jax import lax
from jax.experimental import pallas as pl
from jax.experimental.pallas import tpu as pltpu
from jax.sharding import PartitionSpec as P

NC1_DEV = 256
NC2_DEV = 64
CB1 = 64
CB2 = 32


def ln(pre, gain):
    mean = jnp.mean(pre, axis=-1, keepdims=True)
    c = pre - mean
    var = jnp.mean(c*c, axis=-1, keepdims=True)
    return c * lax.rsqrt(var + 1e-05) * gain

def silu(x):
    return x / (1.0 + jnp.exp(-x))

def dotf(a, b):
    return jnp.dot(a, b, preferred_element_type=jnp.float32)


def make_fine(nodes, edges, feats, bnd, own1, ext1, B=256, sub=256):
    lanes = 128
    C = feats // lanes
    steps = edges // (2*B)
    nsrc = nodes + 9*bnd

    def put(tab, start, val):
        n = val.shape[0]
        for c in range(C):
            tab[pl.ds(start*C + c, n, stride=C), :] = val[:, c*lanes:(c+1)*lanes]

    def kernel(src_ref, dsts_ref, fn_ref, gxm, gxp, gym, gyp, lat_ref, dstv_ref, par_ref, wt_ref,
               win_ref, wout_ref, gain_ref, uin_ref, uout_ref, ugain_ref,
               new_ref, own_ref, blk_ref, tab_s, tab_d, g0, g1, acc):
        i = pl.program_id(0)

        def gather(base, g):
            for j in range(B):
                s = src_ref[base + j]
                d = dsts_ref[base + j]
                g[C*j:C*(j+1), :] = (tab_s[pl.ds(pl.multiple_of(s*C, C), C), :]
                                     + tab_d[pl.ds(pl.multiple_of(d*C, C), C), :])

        @pl.when(i == 0)
        def _():
            ws = win_ref[:feats, :]
            put(tab_s, 0, dotf(fn_ref[...], ws))
            put(tab_d, 0, dotf(fn_ref[...], win_ref[feats:2*feats, :]))
            a = dotf(gym[...], ws); b = dotf(gyp[...], ws)
            for t in range(3):
                put(tab_s, nodes + (3*t)*bnd, a[t*bnd:(t+1)*bnd])
                put(tab_s, nodes + (3*t+2)*bnd, b[t*bnd:(t+1)*bnd])
            put(tab_s, nodes + bnd, dotf(gxm[...], ws))
            put(tab_s, nodes + 7*bnd, dotf(gxp[...], ws))
            acc[...] = jnp.zeros_like(acc)
            gather(0, g0)

        def block(h, g):
            msgs = []
            for r in range(0, B, sub):
                pre = dotf(lat_ref[h*B + r:h*B + r + sub, :], win_ref[2*feats:, :])
                pre = pre + jnp.concatenate(
                    [g[pl.ds(C*r + c, sub, stride=C), :] for c in range(C)], axis=1)
                hid = silu(pre).astype(jnp.bfloat16)
                m = ln(dotf(hid, wout_ref[...]), gain_ref[...].astype(jnp.float32))
                msgs.append(m.astype(jnp.bfloat16))
            msg = jnp.concatenate(msgs, axis=0) if len(msgs) > 1 else msgs[0]
            d = dstv_ref[:, h*B:(h+1)*B]
            for n0 in range(0, nodes, 256):
                oh = (lax.broadcasted_iota(jnp.int32, (256, B), 0) + n0 == d).astype(jnp.bfloat16)
                acc[n0:n0+256, :] += dotf(oh, msg)

        gather((2*i+1)*B, g1)
        block(0, g0)
        gather(jnp.minimum(2*i+2, 2*steps-1)*B, g0)
        block(1, g1)

        @pl.when(i == steps-1)
        def _():
            gain = ugain_ref[...].astype(jnp.float32)
            for n0 in range(0, nodes, 256):
                st = fn_ref[n0:n0+256, :]
                pre = dotf(st, uin_ref[:feats, :]) + dotf(acc[n0:n0+256, :].astype(jnp.bfloat16), uin_ref[feats:, :])
                hid = silu(pre).astype(jnp.bfloat16)
                new_ref[n0:n0+256, :] = (st.astype(jnp.float32) + ln(dotf(hid, uout_ref[...]), gain)).astype(jnp.bfloat16)
            for n0 in range(0, ext1, 64):
                sel = lax.broadcasted_iota(jnp.int32, (64, nodes), 0) + n0 == par_ref[...]
                sm = jnp.where(sel, wt_ref[...].astype(jnp.float32), 0.0).astype(jnp.bfloat16)
                out = dotf(sm, new_ref[...])
                if n0 < own1:
                    own_ref[n0:n0+64, :] = out
                else:
                    blk_ref[n0-own1:n0-own1+64, :] = out.astype(jnp.bfloat16)

    full = lambda *s: pl.BlockSpec(s, lambda i, *_: (0,)*len(s))
    grid_spec = pltpu.PrefetchScalarGridSpec(
        num_scalar_prefetch=2, grid=(steps,),
        in_specs=[full(nodes, feats), full(bnd, feats), full(bnd, feats), full(3*bnd, feats), full(3*bnd, feats),
                  pl.BlockSpec((2*B, feats), lambda i, *_: (i, 0)),
                  pl.BlockSpec((1, 2*B), lambda i, *_: (0, i)),
                  full(1, nodes), full(1, nodes),
                  full(3*feats, feats), full(feats, feats), full(1, feats),
                  full(2*feats, feats), full(feats, feats), full(1, feats)],
        out_specs=[full(nodes, feats), full(own1, feats), full(ext1-own1, feats)],
        scratch_shapes=[pltpu.VMEM((nsrc*C, lanes), jnp.float32), pltpu.VMEM((nodes*C, lanes), jnp.float32),
                        pltpu.VMEM((B*C, lanes), jnp.float32), pltpu.VMEM((B*C, lanes), jnp.float32),
                        pltpu.VMEM((nodes, feats), jnp.float32)])
    return pl.pallas_call(kernel, grid_spec=grid_spec,
        out_shape=[jax.ShapeDtypeStruct((nodes, feats), jnp.bfloat16),
                   jax.ShapeDtypeStruct((own1, feats), jnp.float32),
                   jax.ShapeDtypeStruct((ext1-own1, feats), jnp.bfloat16)],
        compiler_params=pltpu.CompilerParams(dimension_semantics=("arbitrary",), vmem_limit_bytes=60*1024*1024),
        name="fine_stage")


def padded(cells, sides, width):
    for axis, dim in sides:
        count = lax.axis_size(axis)
        head = lax.slice_in_dim(cells, 0, width, axis=dim)
        tail = lax.slice_in_dim(cells, cells.shape[dim] - width, cells.shape[dim], axis=dim)
        cells = jnp.concatenate(
            [
                lax.ppermute(tail, axis, [(i, (i + 1) % count) for i in range(count)]),
                cells,
                lax.ppermute(head, axis, [((i + 1) % count, i) for i in range(count)]),
            ],
            axis=dim,
        )
    return cells


def passed_along(value, axis, steps):
    count = lax.axis_size(axis)
    pairs = [(source, (source + steps) % count) for source in range(count)]
    return lax.ppermute(value, axis, pairs)


def normed(preact, scales):
    average = jnp.mean(preact, axis=-1, keepdims=True)
    centred = preact - average
    spread = jnp.mean(centred * centred, axis=-1, keepdims=True)
    return centred * lax.rsqrt(spread + 1e-05) * scales.astype(jnp.float32)


def finish(preact, project_out, scales):
    hidden = jax.nn.silu(preact).astype(jnp.bfloat16)
    return normed(jnp.dot(hidden, project_out, preferred_element_type=jnp.float32), scales)


def summed(targets, messages, node_count):
    onehot = (lax.iota(jnp.int32, node_count)[:, None] == targets[None, :]).astype(jnp.bfloat16)
    return jnp.dot(onehot, messages, preferred_element_type=jnp.float32)


def node_update(states, incoming, update_in, update_out, update_gain):
    features = states.shape[1]
    preact = jnp.dot(states, update_in[:features], preferred_element_type=jnp.float32)
    preact = preact + jnp.dot(
        incoming.astype(jnp.bfloat16), update_in[features:], preferred_element_type=jnp.float32
    )
    return (states.astype(jnp.float32) + finish(preact, update_out, update_gain)).astype(
        jnp.bfloat16
    )


def extend_rows(owned_rows, rim_count):
    rims = padded(owned_rows[:rim_count][None, None], (("gx", 0), ("gy", 1)), 1)
    return jnp.concatenate([owned_rows, rims.reshape(-1, owned_rows.shape[1])], axis=0)


def lift_rows(coarse_rows, rim_count, parents):
    rims = padded(coarse_rows[:rim_count][None, None], (("gx", 0), ("gy", 1)), 1)
    extended = jnp.concatenate([coarse_rows, rims.reshape(-1, coarse_rows.shape[1])], axis=0)
    return jnp.take(extended, parents, axis=0).astype(jnp.float32)


def coarse_level(
    owned_rows,
    extended,
    sources,
    targets,
    message_in,
    message_out,
    message_gain,
    update_in,
    update_out,
    update_gain,
):
    features = owned_rows.shape[1]
    source_proj = jnp.dot(extended, message_in[:features], preferred_element_type=jnp.float32)
    target_proj = jnp.dot(owned_rows, message_in[features:], preferred_element_type=jnp.float32)
    preact = jnp.take(source_proj, sources, axis=0) + jnp.take(target_proj, targets, axis=0)
    messages = finish(preact, message_out, message_gain).astype(jnp.bfloat16)
    incoming = summed(targets, messages, owned_rows.shape[0])
    return node_update(owned_rows, incoming, update_in, update_out, update_gain)


def gathered_sums(own_sums, beyond, rim_count):
    features = own_sums.shape[1]
    blocks = beyond.reshape(3, 3, rim_count, features)
    column = blocks[:, 1].astype(jnp.float32)
    for step_y in (-1, 1):
        column = column + passed_along(blocks[:, step_y + 1], "gy", step_y).astype(jnp.float32)
    inbound = column[1]
    for step_x in (-1, 1):
        inbound = inbound + passed_along(
            column[step_x + 1].astype(jnp.bfloat16), "gx", step_x
        ).astype(jnp.float32)
    owned = jnp.concatenate([own_sums[:rim_count] + inbound, own_sums[rim_count:]], axis=0)
    return owned.astype(jnp.bfloat16)


def restrict(states, parents, weights, local_count, rim_count):
    positions = lax.iota(jnp.int32, local_count + 9 * rim_count)
    spread_matrix = jnp.where(
        positions[:, None] == parents[None, :], weights[None, :], jnp.zeros((), jnp.bfloat16)
    )
    spread_sums = jnp.dot(spread_matrix, states, preferred_element_type=jnp.float32)
    return gathered_sums(
        spread_sums[:local_count], spread_sums[local_count:].astype(jnp.bfloat16), rim_count
    )


def per_device(
    fine_nodes,
    edge_latent,
    boundary,
    fine_src,
    fine_dst,
    parent_one,
    weight_one,
    coarse_src_one,
    coarse_dst_one,
    parent_two,
    weight_two,
    coarse_src_two,
    coarse_dst_two,
    fine_message_in,
    fine_message_out,
    fine_message_gain,
    fine_update_in,
    fine_update_out,
    fine_update_gain,
    coarse_message_in,
    coarse_message_out,
    coarse_message_gain,
    coarse_update_in,
    coarse_update_out,
    coarse_update_gain,
):
    nodes, features = fine_nodes.shape
    rim = boundary.shape[0]
    pick = (boundary[:, None] == lax.iota(jnp.int32, nodes)[None, :]).astype(jnp.bfloat16)
    edge_rows = dotf(pick, fine_nodes).astype(jnp.bfloat16)
    from_left = passed_along(edge_rows, "gx", 1)
    from_right = passed_along(edge_rows, "gx", -1)
    stack = jnp.concatenate([from_left, edge_rows, from_right], axis=0)
    from_below = passed_along(stack, "gy", 1)
    from_above = passed_along(stack, "gy", -1)
    fine_new, own_sums, beyond = make_fine(
        nodes, edge_latent.shape[0], features, rim, NC1_DEV, NC1_DEV + 9 * CB1, B=512, sub=512
    )(
        fine_src, fine_dst, fine_nodes, from_left, from_right, from_below, from_above,
        edge_latent, fine_dst[None, :], parent_one[None, :], weight_one[None, :],
        fine_message_in, fine_message_out, fine_message_gain[None, :],
        fine_update_in, fine_update_out, fine_update_gain[None, :],
    )
    level_one = gathered_sums(own_sums, beyond, CB1)
    level_one_new = coarse_level(
        level_one,
        extend_rows(level_one, CB1),
        coarse_src_one,
        coarse_dst_one,
        coarse_message_in,
        coarse_message_out,
        coarse_message_gain,
        coarse_update_in,
        coarse_update_out,
        coarse_update_gain,
    )
    level_two = restrict(level_one_new, parent_two, weight_two, NC2_DEV, CB2)
    level_two_new = coarse_level(
        level_two,
        extend_rows(level_two, CB2),
        coarse_src_two,
        coarse_dst_two,
        coarse_message_in,
        coarse_message_out,
        coarse_message_gain,
        coarse_update_in,
        coarse_update_out,
        coarse_update_gain,
    )
    level_one_final = (
        level_one_new.astype(jnp.float32) + lift_rows(level_two_new, CB2, parent_two)
    ).astype(jnp.bfloat16)
    return (fine_new.astype(jnp.float32) + lift_rows(level_one_final, CB1, parent_one)).astype(
        jnp.bfloat16
    )


def solution(mesh):
    in_specs = (
        P(("gx", "gy"), None),
        P(("gx", "gy"), None),
        P(("gx", "gy")),
        P(("gx", "gy")),
        P(("gx", "gy")),
        P(("gx", "gy")),
        P(("gx", "gy")),
        P(("gx", "gy")),
        P(("gx", "gy")),
        P(("gx", "gy")),
        P(("gx", "gy")),
        P(("gx", "gy")),
        P(("gx", "gy")),
        P(),
        P(),
        P(),
        P(),
        P(),
        P(),
        P(),
        P(),
        P(),
        P(),
        P(),
        P(),
    )
    out_specs = P(("gx", "gy"), None)
    return jax.shard_map(
        per_device, mesh=mesh, in_specs=in_specs, out_specs=out_specs, check_vma=False
    )
```

```python
import jax
import jax.numpy as jnp
from jax import lax
from jax.experimental import pallas as pl
from jax.experimental.pallas import tpu as pltpu
from jax.sharding import PartitionSpec as P

NC1_DEV = 256
NC2_DEV = 64
CB1 = 64
CB2 = 32
LANES = 128
VMEM_BYTES = 40 * 1024 * 1024
PART_DTYPE = jnp.float32

VSPEC = pl.BlockSpec(memory_space=pltpu.VMEM)
SSPEC = pl.BlockSpec(memory_space=pltpu.SMEM)


def in_hbm(value):
    return pltpu.with_memory_space_constraint(value, pltpu.HBM)


def whole(*shape):
    return pl.BlockSpec(shape, lambda i, *_: (0,) * len(shape))


def params(grid=False):
    return pltpu.CompilerParams(
        dimension_semantics=("arbitrary",) if grid else None, vmem_limit_bytes=VMEM_BYTES
    )


def passed_along(value, axis, steps):
    count = lax.axis_size(axis)
    pairs = [(source, (source + steps) % count) for source in range(count)]
    return lax.ppermute(value, axis, pairs)


def dotf(a, b):
    return jnp.dot(a, b, preferred_element_type=jnp.float32)


def normed(preact, gain):
    centred = preact - jnp.mean(preact, axis=-1, keepdims=True)
    spread = jnp.mean(centred * centred, axis=-1, keepdims=True)
    return centred * lax.rsqrt(spread + 1e-05) * gain


def silu(value):
    half = 0.5 * value
    return half + half * jnp.tanh(half)


def put_rows(table, start, rows):
    count, features = rows.shape
    C = features // LANES
    for c in range(C):
        table[pl.ds(start * C + c, count, stride=C), :] = rows[:, c * LANES : (c + 1) * LANES]


def get_rows(lines, start, count, C):
    return jnp.concatenate(
        [lines[pl.ds(start * C + c, count, stride=C), :] for c in range(C)], axis=1
    )


def line(table, row, C):
    return table[pl.ds(pl.multiple_of(row * C, C), C), :]


def spread(lines, reads, C):
    for j, read in enumerate(reads):
        lines[C * j : C * (j + 1), :] = read()


def onehot_sum(targets, messages, first, count):
    hits = lax.broadcasted_iota(jnp.int32, (count, messages.shape[0]), 0) + first == targets
    return dotf(hits.astype(jnp.bfloat16), messages)


def update_rows(states, incoming, update_in, update_out, gain):
    features = states.shape[1]
    preact = dotf(states, update_in[:features, :]) + dotf(
        incoming.astype(jnp.bfloat16), update_in[features:, :]
    )
    hidden = silu(preact).astype(jnp.bfloat16)
    return (states.astype(jnp.float32) + normed(dotf(hidden, update_out[...]), gain)).astype(
        jnp.bfloat16
    )


def restrict_into(states, parents, weights, local_count, rim_count, own, up, mid, down):
    total = local_count + 9 * rim_count
    hits = lax.broadcasted_iota(jnp.int32, (total, states.shape[0]), 0) == parents
    spread = jnp.where(hits, weights.astype(jnp.float32), 0.0).astype(jnp.bfloat16)
    sums = dotf(spread, states)
    own[...] = sums[:local_count]
    for dx in range(3):
        for dy, ref in ((0, down), (1, mid), (2, up)):
            k = 3 * dx + dy
            rows = sums[local_count + k * rim_count : local_count + (k + 1) * rim_count]
            if k == 4:
                rows = sums[:rim_count]
            ref[dx * rim_count : (dx + 1) * rim_count, :] = rows.astype(ref.dtype)


def restrict_shapes(local_count, rim_count, features):
    return [
        jax.ShapeDtypeStruct((local_count, features), jnp.float32),
        jax.ShapeDtypeStruct((3 * rim_count, features), jnp.bfloat16),
        jax.ShapeDtypeStruct((3 * rim_count, features), jnp.float32),
        jax.ShapeDtypeStruct((3 * rim_count, features), jnp.bfloat16),
    ]


def edge_start(dst, nodes_in, latent, message_in, block, begin, blocks, part=None):
    nodes, features = nodes_in.shape
    edges = latent.shape[0]
    C = features // LANES
    opening = part is None

    def kernel(dst_ref, node_ref, latent_ref, in_ref, *rest):
        part_ref = rest[0 if opening else 1]
        table, lines0, lines1 = rest[-3:]
        step = pl.program_id(0)

        def gather(at, lines):
            base = (begin + jnp.minimum(at, blocks - 1)) * block
            spread(lines, [lambda j=j: line(table, dst_ref[base + j], C) for j in range(block)], C)

        def project(half, lines):
            rows = slice(half * block, (half + 1) * block)
            part_ref[rows, :] = (
                dotf(latent_ref[rows, :], in_ref[2 * features :, :]) + get_rows(lines, 0, block, C)
            ).astype(part_ref.dtype)

        @pl.when(step == 0)
        def _():
            put_rows(table, 0, dotf(node_ref[...], in_ref[features : 2 * features, :]))
            if opening:
                put_rows(rest[1], 0, dotf(node_ref[...], in_ref[:features, :]))
            gather(0, lines0)

        gather(2 * step + 1, lines1)
        project(0, lines0)
        gather(2 * step + 2, lines0)
        project(1, lines1)

    start = begin // 2
    tile = pl.BlockSpec((2 * block, features), lambda i, *_: (i + start, 0))
    part_shape = jax.ShapeDtypeStruct((edges, features), PART_DTYPE)
    return pl.pallas_call(
        kernel,
        grid_spec=pltpu.PrefetchScalarGridSpec(
            num_scalar_prefetch=1,
            grid=(blocks // 2,),
            in_specs=[whole(nodes, features), tile, whole(3 * features, features)] + ([] if opening else [pl.BlockSpec(memory_space=pl.ANY)]),
            out_specs=[tile, VSPEC] if opening else tile,
            scratch_shapes=[
                pltpu.VMEM((nodes * C, LANES), jnp.float32),
                pltpu.VMEM((block * C, LANES), jnp.float32),
                pltpu.VMEM((block * C, LANES), jnp.float32),
            ],
        ),
        out_shape=[part_shape, jax.ShapeDtypeStruct((nodes * C, LANES), jnp.float32)]
        if opening
        else part_shape,
        input_output_aliases={} if opening else {4: 0},
        compiler_params=params(True),
        cost_estimate=pl.CostEstimate(
            flops=2 * blocks * block * features * features, transcendentals=0,
            bytes_accessed=6 * blocks * block * features,
        ),
        name="edge_start",
    )(in_hbm(dst), in_hbm(nodes_in), in_hbm(latent), in_hbm(message_in), *(() if opening else (in_hbm(part),)))


def fine_stage(src, dst, nodes_in, own_lines, left, right, below, above, part, parents, weights,
               message_in, message_out, message_gain, update_in, update_out, update_gain, block):
    nodes, features = nodes_in.shape
    rim = left.shape[0]
    edges = part.shape[0]
    steps = edges // (2 * block)
    C = features // LANES

    def kernel(src_ref, node_ref, own_ref, left_ref, right_ref, below_ref, above_ref, part_ref,
               dst_ref, parent_ref, weight_ref, in_ref, out_ref, gain_ref, uin_ref, uout_ref,
               ugain_ref, new_ref, sums_ref, up_ref, mid_ref, down_ref, table, lines0, lines1, acc, sent):
        step = pl.program_id(0)

        def gather(base, lines):
            spread(lines, [lambda j=j: line(table, src_ref[base + j], C) for j in range(block)], C)

        @pl.when(step == 0)
        def _():
            table[: nodes * C, :] = own_ref[...]
            first = in_ref[:features, :]
            low, high = dotf(below_ref[...], first), dotf(above_ref[...], first)
            for t in range(3):
                put_rows(table, nodes + 3 * t * rim, low[t * rim : (t + 1) * rim])
                put_rows(table, nodes + (3 * t + 2) * rim, high[t * rim : (t + 1) * rim])
            put_rows(table, nodes + rim, dotf(left_ref[...], first))
            put_rows(table, nodes + 7 * rim, dotf(right_ref[...], first))
            acc[...] = jnp.zeros_like(acc)
            gather(0, lines0)

        def block_sum(half, lines):
            preact = part_ref[half * block : (half + 1) * block, :].astype(jnp.float32) + get_rows(lines, 0, block, C)
            hidden = silu(preact).astype(jnp.bfloat16)
            messages = normed(dotf(hidden, out_ref[...]), gain_ref[...].astype(jnp.float32))
            sent[half * block : (half + 1) * block, :] = messages.astype(jnp.bfloat16)

        gather((2 * step + 1) * block, lines1)
        block_sum(0, lines0)
        gather(jnp.minimum(2 * step + 2, 2 * steps - 1) * block, lines0)
        block_sum(1, lines1)
        for n in range(0, nodes, 256):
            acc[n : n + 256, :] += onehot_sum(dst_ref[...], sent[...], n, 256)

        @pl.when(step == steps - 1)
        def _():
            gain = ugain_ref[...].astype(jnp.float32)
            new_ref[...] = update_rows(node_ref[...], acc[...], uin_ref, uout_ref, gain)
            restrict_into(new_ref[...], parent_ref[...], weight_ref[...], NC1_DEV, CB1,
                          sums_ref, up_ref, mid_ref, down_ref)

    return pl.pallas_call(
        kernel,
        grid_spec=pltpu.PrefetchScalarGridSpec(
            num_scalar_prefetch=1,
            grid=(steps,),
            in_specs=[
                VSPEC, VSPEC, VSPEC, VSPEC, VSPEC, VSPEC,
                pl.BlockSpec((2 * block, features), lambda i, *_: (i, 0)),
                pl.BlockSpec((1, 2 * block), lambda i, *_: (0, i)),
                VSPEC, VSPEC, VSPEC, VSPEC, VSPEC, VSPEC, VSPEC, VSPEC,
            ],
            out_specs=[VSPEC] * 5,
            scratch_shapes=[
                pltpu.VMEM(((nodes + 9 * rim) * C, LANES), jnp.float32),
                pltpu.VMEM((block * C, LANES), jnp.float32),
                pltpu.VMEM((block * C, LANES), jnp.float32),
                pltpu.VMEM((nodes, features), jnp.float32),
                pltpu.VMEM((2 * block, features), jnp.bfloat16),
            ],
        ),
        out_shape=[jax.ShapeDtypeStruct((nodes, features), jnp.bfloat16)]
        + restrict_shapes(NC1_DEV, CB1, features),
        compiler_params=params(True),
        name="fine_stage",
    )(src, nodes_in, own_lines, left, right, below, above, in_hbm(part), dst[None, :], parents, weights,
      message_in, message_out, message_gain, update_in, update_out, update_gain)


def column_sums(mid, from_below, from_above):
    rim, features = mid.shape[0] // 3, mid.shape[1]

    def kernel(mid_ref, below_ref, above_ref, right_ref, left_ref, far_right_ref, far_left_ref):
        total = (
            mid_ref[...] + below_ref[...].astype(jnp.float32) + above_ref[...].astype(jnp.float32)
        ).astype(jnp.bfloat16)
        right_ref[...] = total[rim:]
        left_ref[...] = total[: 2 * rim]
        far_right_ref[...] = total[2 * rim :]
        far_left_ref[...] = total[:rim]

    return pl.pallas_call(
        kernel,
        in_specs=[VSPEC] * 3,
        out_specs=[VSPEC] * 4,
        out_shape=[jax.ShapeDtypeStruct((n * rim, features), jnp.bfloat16) for n in (2, 2, 1, 1)],
        compiler_params=params(),
        name="column_sums",
    )(mid, from_below, from_above)


def rim_sums(right, left, in_left, in_right, in_far_left, in_far_right):
    rim, features = right.shape[0] // 2, right.shape[1]

    def kernel(right_ref, left_ref, a1, b1, a2, b2, out_ref):
        def add(*parts):
            total = parts[0].astype(jnp.float32)
            for part in parts[1:]:
                total = total + part.astype(jnp.float32)
            return total.astype(jnp.bfloat16)

        out_ref[:rim, :] = add(a1[:rim, :], a2[...], left_ref[:rim, :])
        out_ref[rim : 2 * rim, :] = add(right_ref[:rim, :], a1[rim:, :], b1[:rim, :])
        out_ref[2 * rim :, :] = add(b1[rim:, :], b2[...], right_ref[rim:, :])

    return pl.pallas_call(
        kernel,
        in_specs=[VSPEC] * 6,
        out_specs=VSPEC,
        out_shape=jax.ShapeDtypeStruct((3 * rim, features), jnp.bfloat16),
        compiler_params=params(),
        name="rim_sums",
    )(right, left, in_left, in_right, in_far_left, in_far_right)


def shared_rims(up, mid, down):
    from_below = passed_along(up, "gy", 1)
    from_above = passed_along(down, "gy", -1)
    right, left, far_right, far_left = column_sums(mid, from_below, from_above)
    in_left = passed_along(right, "gx", 1)
    in_right = passed_along(left, "gx", -1)
    in_far_left = passed_along(far_right, "gx", 2)
    in_far_right = passed_along(far_left, "gx", -2)
    rims = rim_sums(right, left, in_left, in_right, in_far_left, in_far_right)
    return rims, passed_along(rims, "gy", 1), passed_along(rims, "gy", -1)


def put_extended(table, local_count, rim_count, line_rows, below_rows, above_rows):
    for t in range(3):
        span = slice(t * rim_count, (t + 1) * rim_count)
        put_rows(table, local_count + 3 * t * rim_count, below_rows[span])
        if t != 1:
            put_rows(table, local_count + (3 * t + 1) * rim_count, line_rows[span])
        put_rows(table, local_count + (3 * t + 2) * rim_count, above_rows[span])


def level_pass(sums, rims, below, above, src, dst, parents, weights, message_in, message_out,
               message_gain, update_in, update_out, update_gain, chunk, block, below_level):
    count, features = sums.shape
    rim = rims.shape[0] // 3
    edges = src.shape[0]
    C = features // LANES

    def kernel(sums_ref, rims_ref, below_ref, above_ref, src_ref, dst_ref, dstv_ref, parent_ref,
               weight_ref, in_ref, out_ref, gain_ref, uin_ref, uout_ref, ugain_ref, *rest):
        outs, (level, table, targets, lines) = rest[:-4], rest[-4:]
        level[:rim, :] = rims_ref[rim : 2 * rim, :]
        level[rim:, :] = sums_ref[rim:, :].astype(jnp.bfloat16)
        first = in_ref[:features, :]
        put_rows(table, 0, dotf(level[...], first))
        put_rows(targets, 0, dotf(level[...], in_ref[features:, :]))
        put_extended(table, count, rim, dotf(rims_ref[...], first), dotf(below_ref[...], first),
                     dotf(above_ref[...], first))

        @pl.loop(0, edges // chunk)
        def _(t):
            for j in range(chunk):
                e = t * chunk + j
                lines[pl.ds(pl.multiple_of(e * C, C), C), :] = line(
                    table, src_ref[e], C
                ) + line(targets, dst_ref[e], C)

        incoming = jnp.zeros((count, features), jnp.float32)
        for start in range(0, edges, block):
            hidden = silu(get_rows(lines, start, block, C)).astype(jnp.bfloat16)
            messages = normed(dotf(hidden, out_ref[...]), gain_ref[...].astype(jnp.float32))
            incoming = incoming + onehot_sum(
                dstv_ref[:, start : start + block], messages.astype(jnp.bfloat16), 0, count
            )
        new = update_rows(level[...], incoming, uin_ref, uout_ref,
                          ugain_ref[...].astype(jnp.float32))
        outs[0][...] = new
        if below_level:
            restrict_into(new, parent_ref[...], weight_ref[...], *below_level, *outs[1:])
        else:
            outs[1][...] = new[:rim]

    shapes = [jax.ShapeDtypeStruct((count, features), jnp.bfloat16)]
    if below_level:
        shapes += restrict_shapes(*below_level, features)
    else:
        shapes += [jax.ShapeDtypeStruct((rim, features), jnp.bfloat16)]
    return pl.pallas_call(
        kernel,
        in_specs=[VSPEC] * 4 + [SSPEC] * 2 + [VSPEC] * 9,
        out_specs=[VSPEC] * len(shapes),
        out_shape=shapes,
        scratch_shapes=[
            pltpu.VMEM((count, features), jnp.bfloat16),
            pltpu.VMEM(((count + 9 * rim) * C, LANES), jnp.float32),
            pltpu.VMEM((count * C, LANES), jnp.float32),
            pltpu.VMEM((edges * C, LANES), jnp.float32),
        ],
        compiler_params=params(),
        name="level_pass",
    )(sums, rims, below, above, src, dst, dst[None, :], parents, weights, message_in, message_out,
      message_gain, update_in, update_out, update_gain)


def lifted(coarse, rims, below, above, parents, states, chunk, rim_out):
    count, features = states.shape
    local_count = coarse.shape[0]
    rim = rims.shape[0] // 3
    C = features // LANES

    def kernel(coarse_ref, rims_ref, below_ref, above_ref, parent_ref, state_ref, *rest):
        outs, (table, lines) = rest[:-2], rest[-2:]
        put_rows(table, 0, coarse_ref[...].astype(jnp.float32))
        put_extended(table, local_count, rim, rims_ref[...].astype(jnp.float32),
                     below_ref[...].astype(jnp.float32), above_ref[...].astype(jnp.float32))

        @pl.loop(0, count // chunk)
        def _(t):
            for j in range(chunk):
                e = t * chunk + j
                lines[pl.ds(pl.multiple_of(e * C, C), C), :] = line(table, parent_ref[e], C)

        result = (state_ref[...].astype(jnp.float32) + get_rows(lines, 0, count, C)).astype(
            jnp.bfloat16
        )
        outs[0][...] = result
        if rim_out:
            outs[1][...] = result[:rim_out]

    shapes = [jax.ShapeDtypeStruct((count, features), jnp.bfloat16)]
    if rim_out:
        shapes.append(jax.ShapeDtypeStruct((rim_out, features), jnp.bfloat16))
    return pl.pallas_call(
        kernel,
        in_specs=[VSPEC] * 4 + [SSPEC, VSPEC],
        out_specs=[VSPEC] * len(shapes),
        out_shape=shapes,
        scratch_shapes=[
            pltpu.VMEM(((local_count + 9 * rim) * C, LANES), jnp.float32),
            pltpu.VMEM((count * C, LANES), jnp.float32),
        ],
        compiler_params=params(),
        name="lifted",
    )(coarse, rims, below, above, parents, states)


def halo(rows):
    left = passed_along(rows, "gx", 1)
    right = passed_along(rows, "gx", -1)
    stack = jnp.concatenate([left, rows, right], axis=0)
    return left, right, stack, passed_along(stack, "gy", 1), passed_along(stack, "gy", -1)


def per_device(
    fine_nodes,
    edge_latent,
    boundary,
    fine_src,
    fine_dst,
    parent_one,
    weight_one,
    coarse_src_one,
    coarse_dst_one,
    parent_two,
    weight_two,
    coarse_src_two,
    coarse_dst_two,
    fine_message_in,
    fine_message_out,
    fine_message_gain,
    fine_update_in,
    fine_update_out,
    fine_update_gain,
    coarse_message_in,
    coarse_message_out,
    coarse_message_gain,
    coarse_update_in,
    coarse_update_out,
    coarse_update_gain,
):
    nodes, features = fine_nodes.shape
    pick = (boundary[:, None] == lax.iota(jnp.int32, nodes)[None, :]).astype(jnp.bfloat16)
    edge_rows = dotf(pick, fine_nodes).astype(jnp.bfloat16)
    half = edge_latent.shape[0] // 1024
    left = passed_along(edge_rows, "gx", 1)
    right = passed_along(edge_rows, "gx", -1)
    part, own_lines = edge_start(fine_dst, fine_nodes, edge_latent, fine_message_in, 512, 0, half)
    left, right, part = lax.optimization_barrier((left, right, part))
    stack = jnp.concatenate([left, edge_rows, right], axis=0)
    below = passed_along(stack, "gy", 1)
    above = passed_along(stack, "gy", -1)
    part = edge_start(
        fine_dst, fine_nodes, edge_latent, fine_message_in, 512, half, half, part
    )
    fine_new, sums, up, mid, down = fine_stage(
        fine_src, fine_dst, fine_nodes, own_lines, left, right, below, above, part,
        parent_one[None, :], weight_one[None, :], fine_message_in, fine_message_out,
        fine_message_gain[None, :], fine_update_in, fine_update_out, fine_update_gain[None, :], 512,
    )
    coarse = (
        coarse_message_in, coarse_message_out, coarse_message_gain[None, :],
        coarse_update_in, coarse_update_out, coarse_update_gain[None, :],
    )
    rims, below, above = shared_rims(up, mid, down)
    level_one_new, sums, up, mid, down = level_pass(
        sums, rims, below, above, coarse_src_one, coarse_dst_one, parent_two[None, :],
        weight_two[None, :], *coarse, 128, 512, (NC2_DEV, CB2),
    )
    rims, below, above = shared_rims(up, mid, down)
    level_two_new, rim_two = level_pass(
        sums, rims, below, above, coarse_src_two, coarse_dst_two, parent_two[None, :],
        weight_two[None, :], *coarse, 128, coarse_src_two.shape[0], None,
    )
    _, _, stack, below, above = halo(rim_two)
    level_one_final, rim_one = lifted(
        level_two_new, stack, below, above, parent_two, level_one_new, 128, CB1
    )
    _, _, stack, below, above = halo(rim_one)
    return lifted(level_one_final, stack, below, above, parent_one, fine_new, 128, 0)[0]


def solution(mesh):
    rows, flat, copied = P(("gx", "gy"), None), P(("gx", "gy")), P()
    in_specs = (rows, rows) + (flat,) * 11 + (copied,) * 12
    return jax.shard_map(
        per_device, mesh=mesh, in_specs=in_specs, out_specs=rows, check_vma=False
    )
```

```python
import jax
import jax.numpy as jnp
from jax import lax
from jax.experimental import pallas as pl
from jax.experimental.pallas import tpu as pltpu
from jax.sharding import PartitionSpec as P

NC1_DEV = 256
NC2_DEV = 64
CB1 = 64
CB2 = 32
LANES = 128
VMEM_BYTES = 40 * 1024 * 1024
PART_DTYPE = jnp.bfloat16
ROWS = 512

VSPEC = pl.BlockSpec(memory_space=pltpu.VMEM)
SSPEC = pl.BlockSpec(memory_space=pltpu.SMEM)


def in_hbm(value):
    return pltpu.with_memory_space_constraint(value, pltpu.HBM)


def whole(*shape):
    return pl.BlockSpec(shape, lambda i, *_: (0,) * len(shape))


def params(grid=False):
    return pltpu.CompilerParams(
        dimension_semantics=("arbitrary",) if grid else None, vmem_limit_bytes=VMEM_BYTES,
    )


def passed_along(value, axis, steps):
    count = lax.axis_size(axis)
    pairs = [(source, (source + steps) % count) for source in range(count)]
    return lax.ppermute(value, axis, pairs)


def dotf(a, b):
    return jnp.dot(a, b, preferred_element_type=jnp.float32)


def normed(preact, gain):
    centred = preact - jnp.mean(preact, axis=-1, keepdims=True)
    spread = jnp.mean(centred * centred, axis=-1, keepdims=True)
    return centred * lax.rsqrt(spread + 1e-05) * gain


def silu(value):
    half = 0.5 * value
    return half + half * jnp.tanh(half)


def put_rows(table, start, rows):
    count, features = rows.shape
    C = features // LANES
    for c in range(C):
        table[pl.ds(start * C + c, count, stride=C), :] = rows[:, c * LANES : (c + 1) * LANES]


def get_rows(lines, start, count, C):
    return jnp.concatenate(
        [lines[pl.ds(start * C + c, count, stride=C), :] for c in range(C)], axis=1
    )


def line(table, row, C):
    return table[pl.ds(pl.multiple_of(row * C, C), C), :]


def onehot_sum(targets, messages, first, count):
    hits = lax.broadcasted_iota(jnp.int32, (count, messages.shape[0]), 0) + first == targets
    return dotf(hits.astype(jnp.bfloat16), messages)


def update_rows(states, incoming, update_in, update_out, gain):
    features = states.shape[1]
    preact = dotf(states, update_in[:features, :]) + dotf(
        incoming.astype(jnp.bfloat16), update_in[features:, :]
    )
    hidden = silu(preact).astype(jnp.bfloat16)
    return (states.astype(jnp.float32) + normed(dotf(hidden, update_out[...]), gain)).astype(
        jnp.bfloat16
    )


def restrict_into(states, parents, weights, local_count, rim_count, own, up, mid, down):
    total = local_count + 9 * rim_count
    hits = lax.broadcasted_iota(jnp.int32, (total, states.shape[0]), 0) == parents
    spread = jnp.where(hits, weights.astype(jnp.float32), 0.0).astype(jnp.bfloat16)
    sums = dotf(spread, states)
    own[...] = sums[:local_count]
    for dx in range(3):
        for dy, ref in ((0, down), (1, mid), (2, up)):
            k = 3 * dx + dy
            rows = sums[local_count + k * rim_count : local_count + (k + 1) * rim_count]
            if k == 4:
                rows = sums[:rim_count]
            ref[dx * rim_count : (dx + 1) * rim_count, :] = rows.astype(ref.dtype)


def restrict_shapes(local_count, rim_count, features):
    return [
        jax.ShapeDtypeStruct((local_count, features), jnp.float32),
        jax.ShapeDtypeStruct((3 * rim_count, features), jnp.bfloat16),
        jax.ShapeDtypeStruct((3 * rim_count, features), jnp.float32),
        jax.ShapeDtypeStruct((3 * rim_count, features), jnp.bfloat16),
    ]


def edge_start(dst, nodes_in, latent, message_in, block, begin, blocks, part=None, table_in=None):
    nodes, features = nodes_in.shape
    edges = latent.shape[0]
    C = features // LANES
    opening = part is None

    def kernel(dst_ref, latent_ref, last_ref, first_in, second_in, *rest):
        if opening:
            third_in, part_ref, source_ref, table = rest[:4]
        else:
            table, part_ref = first_in, rest[0]
        lines0, lines1 = rest[-2:]
        step = pl.program_id(0)

        @pl.when(step == 0)
        def _():
            if opening:
                put_rows(table, 0, dotf(first_in[...], third_in[...]))
                put_rows(source_ref, 0, dotf(first_in[...], second_in[...]))

        base = (begin + 2 * step) * block
        for half, lines in ((0, lines0), (1, lines1)):
            rows = slice(half * block, (half + 1) * block)
            value = dotf(latent_ref[rows, :], last_ref[...])
            for j in range(block):
                lines[C * j : C * (j + 1), :] = line(table, dst_ref[base + half * block + j], C)
            part_ref[rows, :] = (value + get_rows(lines, 0, block, C)).astype(part_ref.dtype)

    start = begin // 2
    tile = pl.BlockSpec((2 * block, features), lambda i, *_: (i + start, 0))
    weights = [pl.BlockSpec((features, features), lambda i, *_, p=p: (p, 0)) for p in range(3)]
    part_shape = jax.ShapeDtypeStruct((edges, features), PART_DTYPE)
    lines_shape = jax.ShapeDtypeStruct((nodes * C, LANES), jnp.float32)
    if opening:
        more, specs = [in_hbm(nodes_in)] + [in_hbm(message_in)] * 2, [whole(nodes, features)] + weights[:2]
    else:
        more, specs = [table_in, in_hbm(part)], [VSPEC, pl.BlockSpec(memory_space=pl.ANY)]
    return pl.pallas_call(
        kernel,
        grid_spec=pltpu.PrefetchScalarGridSpec(
            num_scalar_prefetch=1,
            grid=(blocks // 2,),
            in_specs=[tile, weights[2]] + specs,
            out_specs=[tile, VSPEC, VSPEC] if opening else tile,
            scratch_shapes=[pltpu.VMEM((block * C, LANES), jnp.float32)] * 2,
        ),
        out_shape=[part_shape, lines_shape, lines_shape] if opening else part_shape,
        input_output_aliases={} if opening else {4: 0},
        compiler_params=params(True),
        cost_estimate=pl.CostEstimate(
            flops=2 * blocks * block * features * features, transcendentals=0,
            bytes_accessed=6 * blocks * block * features,
        ),
        name="edge_start",
    )(in_hbm(dst), in_hbm(latent), in_hbm(message_in), *more)


def fine_stage(src, dst, nodes_in, own_lines, left, right, below, above, part, parents, weights,
               message_in, message_out, message_gain, update_in, update_out, update_gain, block):
    nodes, features = nodes_in.shape
    rim = left.shape[0]
    edges = part.shape[0]
    steps = edges // (2 * block)
    C = features // LANES

    def kernel(src_ref, node_ref, own_ref, left_ref, right_ref, below_ref, above_ref, part_ref,
               dst_ref, parent_ref, weight_ref, in_ref, out_ref, gain_ref, uin_ref, uout_ref,
               ugain_ref, new_ref, sums_ref, up_ref, mid_ref, down_ref, table, lines0, lines1, acc, sent):
        step = pl.program_id(0)

        def gather(base, lines, first, count):
            for j in range(first, first + count):
                lines[C * j : C * (j + 1), :] = line(table, src_ref[base + j], C)

        @pl.when(step == 0)
        def _():
            table[: nodes * C, :] = own_ref[...]
            first = in_ref[:features, :]
            low, high = dotf(below_ref[...], first), dotf(above_ref[...], first)
            for t in range(3):
                put_rows(table, nodes + 3 * t * rim, low[t * rim : (t + 1) * rim])
                put_rows(table, nodes + (3 * t + 2) * rim, high[t * rim : (t + 1) * rim])
            put_rows(table, nodes + rim, dotf(left_ref[...], first))
            put_rows(table, nodes + 7 * rim, dotf(right_ref[...], first))
            acc[...] = jnp.zeros_like(acc)
            gather(0, lines0, 0, block)
            gather(block, lines1, 0, block)

        def block_sum(half, lines):
            preact = part_ref[half * block : (half + 1) * block, :].astype(jnp.float32) + get_rows(lines, 0, block, C)
            hidden = silu(preact).astype(jnp.bfloat16)
            messages = normed(dotf(hidden, out_ref[...]), gain_ref[...].astype(jnp.float32))
            sent[half * block : (half + 1) * block, :] = messages.astype(jnp.bfloat16)

        block_sum(0, lines0)
        block_sum(1, lines1)
        later = jnp.minimum(step + 1, steps - 1) * 2 * block
        pieces = nodes // ROWS
        for t in range(pieces):
            lines, base = (lines0, later) if 2 * t < pieces else (lines1, later + block)
            span = 2 * block // pieces
            gather(base, lines, (t * span) % block, span)
            acc[t * ROWS : (t + 1) * ROWS, :] += onehot_sum(dst_ref[...], sent[...], t * ROWS, ROWS)

        @pl.when(step == steps - 1)
        def _():
            gain = ugain_ref[...].astype(jnp.float32)
            new_ref[...] = update_rows(node_ref[...], acc[...], uin_ref, uout_ref, gain)
            restrict_into(new_ref[...], parent_ref[...], weight_ref[...], NC1_DEV, CB1,
                          sums_ref, up_ref, mid_ref, down_ref)

    return pl.pallas_call(
        kernel,
        grid_spec=pltpu.PrefetchScalarGridSpec(
            num_scalar_prefetch=1,
            grid=(steps,),
            in_specs=[
                VSPEC, VSPEC, VSPEC, VSPEC, VSPEC, VSPEC,
                pl.BlockSpec((2 * block, features), lambda i, *_: (i, 0)),
                pl.BlockSpec((1, 2 * block), lambda i, *_: (0, i)),
                VSPEC, VSPEC, VSPEC, VSPEC, VSPEC, VSPEC, VSPEC, VSPEC,
            ],
            out_specs=[VSPEC] * 5,
            scratch_shapes=[
                pltpu.VMEM(((nodes + 9 * rim) * C, LANES), jnp.float32),
                pltpu.VMEM((block * C, LANES), jnp.float32),
                pltpu.VMEM((block * C, LANES), jnp.float32),
                pltpu.VMEM((nodes, features), jnp.float32),
                pltpu.VMEM((2 * block, features), jnp.bfloat16),
            ],
        ),
        out_shape=[jax.ShapeDtypeStruct((nodes, features), jnp.bfloat16)]
        + restrict_shapes(NC1_DEV, CB1, features),
        compiler_params=params(True),
        name="fine_stage",
    )(src, nodes_in, own_lines, left, right, below, above, in_hbm(part), dst[None, :], parents, weights,
      message_in, message_out, message_gain, update_in, update_out, update_gain)


def column_sums(mid, from_below, from_above):
    rim, features = mid.shape[0] // 3, mid.shape[1]

    def kernel(mid_ref, below_ref, above_ref, right_ref, left_ref, far_right_ref, far_left_ref):
        total = (
            mid_ref[...] + below_ref[...].astype(jnp.float32) + above_ref[...].astype(jnp.float32)
        ).astype(jnp.bfloat16)
        right_ref[...] = total[rim:]
        left_ref[...] = total[: 2 * rim]
        far_right_ref[...] = total[2 * rim :]
        far_left_ref[...] = total[:rim]

    return pl.pallas_call(
        kernel,
        in_specs=[VSPEC] * 3,
        out_specs=[VSPEC] * 4,
        out_shape=[jax.ShapeDtypeStruct((n * rim, features), jnp.bfloat16) for n in (2, 2, 1, 1)],
        compiler_params=params(),
        name="column_sums",
    )(mid, from_below, from_above)


def rim_sums(right, left, in_left, in_right, in_far_left, in_far_right):
    rim, features = right.shape[0] // 2, right.shape[1]

    def kernel(right_ref, left_ref, a1, b1, a2, b2, out_ref):
        def add(*parts):
            total = parts[0].astype(jnp.float32)
            for part in parts[1:]:
                total = total + part.astype(jnp.float32)
            return total.astype(jnp.bfloat16)

        out_ref[:rim, :] = add(a1[:rim, :], a2[...], left_ref[:rim, :])
        out_ref[rim : 2 * rim, :] = add(right_ref[:rim, :], a1[rim:, :], b1[:rim, :])
        out_ref[2 * rim :, :] = add(b1[rim:, :], b2[...], right_ref[rim:, :])

    return pl.pallas_call(
        kernel,
        in_specs=[VSPEC] * 6,
        out_specs=VSPEC,
        out_shape=jax.ShapeDtypeStruct((3 * rim, features), jnp.bfloat16),
        compiler_params=params(),
        name="rim_sums",
    )(right, left, in_left, in_right, in_far_left, in_far_right)


def shared_rims(up, mid, down):
    from_below = passed_along(up, "gy", 1)
    from_above = passed_along(down, "gy", -1)
    right, left, far_right, far_left = column_sums(mid, from_below, from_above)
    in_left = passed_along(right, "gx", 1)
    in_right = passed_along(left, "gx", -1)
    in_far_left = passed_along(far_right, "gx", 2)
    in_far_right = passed_along(far_left, "gx", -2)
    rims = rim_sums(right, left, in_left, in_right, in_far_left, in_far_right)
    return rims, passed_along(rims, "gy", 1), passed_along(rims, "gy", -1)


def put_extended(table, local_count, rim_count, line_rows, below_rows, above_rows):
    for t in range(3):
        span = slice(t * rim_count, (t + 1) * rim_count)
        put_rows(table, local_count + 3 * t * rim_count, below_rows[span])
        if t != 1:
            put_rows(table, local_count + (3 * t + 1) * rim_count, line_rows[span])
        put_rows(table, local_count + (3 * t + 2) * rim_count, above_rows[span])


def level_pass(sums, rims, below, above, src, dst, parents, weights, message_in, message_out,
               message_gain, update_in, update_out, update_gain, chunk, block, below_level):
    count, features = sums.shape
    rim = rims.shape[0] // 3
    edges = src.shape[0]
    C = features // LANES

    def kernel(sums_ref, rims_ref, below_ref, above_ref, src_ref, dst_ref, dstv_ref, parent_ref,
               weight_ref, in_ref, out_ref, gain_ref, uin_ref, uout_ref, ugain_ref, *rest):
        outs, (level, table, targets, lines) = rest[:-4], rest[-4:]
        level[:rim, :] = rims_ref[rim : 2 * rim, :]
        level[rim:, :] = sums_ref[rim:, :].astype(jnp.bfloat16)
        first = in_ref[:features, :]
        put_rows(table, 0, dotf(level[...], first))
        put_rows(targets, 0, dotf(level[...], in_ref[features:, :]))
        put_extended(table, count, rim, dotf(rims_ref[...], first), dotf(below_ref[...], first),
                     dotf(above_ref[...], first))

        @pl.loop(0, edges // chunk)
        def _(t):
            for j in range(chunk):
                e = t * chunk + j
                lines[pl.ds(pl.multiple_of(e * C, C), C), :] = line(
                    table, src_ref[e], C
                ) + line(targets, dst_ref[e], C)

        incoming = jnp.zeros((count, features), jnp.float32)
        for start in range(0, edges, block):
            hidden = silu(get_rows(lines, start, block, C)).astype(jnp.bfloat16)
            messages = normed(dotf(hidden, out_ref[...]), gain_ref[...].astype(jnp.float32))
            incoming = incoming + onehot_sum(
                dstv_ref[:, start : start + block], messages.astype(jnp.bfloat16), 0, count
            )
        new = update_rows(level[...], incoming, uin_ref, uout_ref,
                          ugain_ref[...].astype(jnp.float32))
        outs[0][...] = new
        if below_level:
            restrict_into(new, parent_ref[...], weight_ref[...], *below_level, *outs[1:])
        else:
            outs[1][...] = new[:rim]

    shapes = [jax.ShapeDtypeStruct((count, features), jnp.bfloat16)]
    if below_level:
        shapes += restrict_shapes(*below_level, features)
    else:
        shapes += [jax.ShapeDtypeStruct((rim, features), jnp.bfloat16)]
    return pl.pallas_call(
        kernel,
        in_specs=[VSPEC] * 4 + [SSPEC] * 2 + [VSPEC] * 9,
        out_specs=[VSPEC] * len(shapes),
        out_shape=shapes,
        scratch_shapes=[
            pltpu.VMEM((count, features), jnp.bfloat16),
            pltpu.VMEM(((count + 9 * rim) * C, LANES), jnp.float32),
            pltpu.VMEM((count * C, LANES), jnp.float32),
            pltpu.VMEM((edges * C, LANES), jnp.float32),
        ],
        compiler_params=params(),
        name="level_pass",
    )(sums, rims, below, above, src, dst, dst[None, :], parents, weights, message_in, message_out,
      message_gain, update_in, update_out, update_gain)


def lifted(coarse, rims, below, above, parents, states, chunk, rim_out):
    count, features = states.shape
    local_count = coarse.shape[0]
    rim = rims.shape[0] // 3
    C = features // LANES

    def kernel(coarse_ref, rims_ref, below_ref, above_ref, parent_ref, state_ref, *rest):
        outs, (table, lines) = rest[:-2], rest[-2:]
        put_rows(table, 0, coarse_ref[...].astype(jnp.float32))
        put_extended(table, local_count, rim, rims_ref[...].astype(jnp.float32),
                     below_ref[...].astype(jnp.float32), above_ref[...].astype(jnp.float32))

        @pl.loop(0, count // chunk)
        def _(t):
            for j in range(chunk):
                e = t * chunk + j
                lines[pl.ds(pl.multiple_of(e * C, C), C), :] = line(table, parent_ref[e], C)

        result = (state_ref[...].astype(jnp.float32) + get_rows(lines, 0, count, C)).astype(
            jnp.bfloat16
        )
        outs[0][...] = result
        if rim_out:
            outs[1][...] = result[:rim_out]

    shapes = [jax.ShapeDtypeStruct((count, features), jnp.bfloat16)]
    if rim_out:
        shapes.append(jax.ShapeDtypeStruct((rim_out, features), jnp.bfloat16))
    return pl.pallas_call(
        kernel,
        in_specs=[VSPEC] * 4 + [SSPEC, VSPEC],
        out_specs=[VSPEC] * len(shapes),
        out_shape=shapes,
        scratch_shapes=[
            pltpu.VMEM(((local_count + 9 * rim) * C, LANES), jnp.float32),
            pltpu.VMEM((count * C, LANES), jnp.float32),
        ],
        compiler_params=params(),
        name="lifted",
    )(coarse, rims, below, above, parents, states)


def halo(rows):
    left = passed_along(rows, "gx", 1)
    right = passed_along(rows, "gx", -1)
    stack = jnp.concatenate([left, rows, right], axis=0)
    return left, right, stack, passed_along(stack, "gy", 1), passed_along(stack, "gy", -1)


def per_device(
    fine_nodes,
    edge_latent,
    boundary,
    fine_src,
    fine_dst,
    parent_one,
    weight_one,
    coarse_src_one,
    coarse_dst_one,
    parent_two,
    weight_two,
    coarse_src_two,
    coarse_dst_two,
    fine_message_in,
    fine_message_out,
    fine_message_gain,
    fine_update_in,
    fine_update_out,
    fine_update_gain,
    coarse_message_in,
    coarse_message_out,
    coarse_message_gain,
    coarse_update_in,
    coarse_update_out,
    coarse_update_gain,
):
    nodes, features = fine_nodes.shape
    pick = (boundary[:, None] == lax.iota(jnp.int32, nodes)[None, :]).astype(jnp.bfloat16)
    edge_rows = dotf(pick, fine_nodes).astype(jnp.bfloat16)
    blocks = edge_latent.shape[0] // 512
    early = blocks // 3 // 2 * 2
    left = passed_along(edge_rows, "gx", 1)
    right = passed_along(edge_rows, "gx", -1)
    part, own_lines, targets = edge_start(
        fine_dst, fine_nodes, edge_latent, fine_message_in, 512, 0, early
    )
    left, right, part = lax.optimization_barrier((left, right, part))
    stack = jnp.concatenate([left, edge_rows, right], axis=0)
    below = passed_along(stack, "gy", 1)
    above = passed_along(stack, "gy", -1)
    part = edge_start(
        fine_dst, fine_nodes, edge_latent, fine_message_in, 512, early, blocks - early, part, targets
    )
    fine_new, sums, up, mid, down = fine_stage(
        fine_src, fine_dst, fine_nodes, own_lines, left, right, below, above, part,
        parent_one[None, :], weight_one[None, :], fine_message_in, fine_message_out,
        fine_message_gain[None, :], fine_update_in, fine_update_out, fine_update_gain[None, :], 512,
    )
    coarse = (
        coarse_message_in, coarse_message_out, coarse_message_gain[None, :],
        coarse_update_in, coarse_update_out, coarse_update_gain[None, :],
    )
    rims, below, above = shared_rims(up, mid, down)
    level_one_new, sums, up, mid, down = level_pass(
        sums, rims, below, above, coarse_src_one, coarse_dst_one, parent_two[None, :],
        weight_two[None, :], *coarse, 128, 512, (NC2_DEV, CB2),
    )
    rims, below, above = shared_rims(up, mid, down)
    level_two_new, rim_two = level_pass(
        sums, rims, below, above, coarse_src_two, coarse_dst_two, parent_two[None, :],
        weight_two[None, :], *coarse, 128, coarse_src_two.shape[0], None,
    )
    _, _, stack, below, above = halo(rim_two)
    level_one_final, rim_one = lifted(
        level_two_new, stack, below, above, parent_two, level_one_new, 128, CB1
    )
    _, _, stack, below, above = halo(rim_one)
    return lifted(level_one_final, stack, below, above, parent_one, fine_new, 128, 0)[0]


def solution(mesh):
    rows, flat, copied = P(("gx", "gy"), None), P(("gx", "gy")), P()
    in_specs = (rows, rows) + (flat,) * 11 + (copied,) * 12
    return jax.shard_map(
        per_device, mesh=mesh, in_specs=in_specs, out_specs=rows, check_vma=False
    )
```
